32 devices in a mesh: row: 4 (over y, x), col: 8 (over z, core).
Axes of the slice: x: 2, y: 2, z: 4, core: 2. Of those that a mesh axis runs over, the one named last changes fastest.
Arguments:
- features: float32 [8, 1536, 256], P('col', 'row'), may hold values from -1000 to 1000
- tiles: bfloat16 [8, 4, 8, 9, 128, 128], P('col', 'row'), may hold values from -0.1875 to 0.1875
- tile_ids: int32 [8, 4, 8, 9], P('col', 'row'), may hold values from 0 to 35
- tile_counts: int32 [8, 4, 8], P('col', 'row'), may hold values from 1 to 9, as said below
Outputs:
- propagated: float32 [8, 1536, 256], P('col', 'row')
- residual_norms: float32 [3], replicated
The draws below stay inside these ranges and needn't reach their ends.
Inputs may be any that keep to these rules, and one draw needn't show every extreme that they name: `tile_ids`: each id is a row tile times 3 plus a column tile; ids may repeat within a list. `tile_counts`: slots at or after the count hold values to be ignored; in every draw some device has 9 live slots for some source block.
All inputs are finite; a program needn't handle non-finite values.
Results may differ from the reference program's by a relative error of at most 0.014.
Values may be sent and summed in bfloat16 or wider, within the bound.
A program may use at most 64 MiB of HBM per device.

```python
import jax
import jax.numpy as jnp
from jax import lax

F = 256
TILE = 128
ITERS = 3
NODE_DEV = 384
COARSE = 8
GROUPS_R = 4
FINE = 1536
ROW_TILES = 12
COL_TILES = 3
SLOTS = 9


def draw_features(key, part):
    keys = jax.random.split(jax.random.fold_in(key, 11), 3)
    row_scale = jnp.exp(jax.random.uniform(keys[1], (COARSE, FINE, 1), jnp.float32, -1.2, 1.2))
    col_scale = jnp.exp(jax.random.uniform(keys[2], (1, 1, F), jnp.float32, -1.2, 1.2))
    inner = jnp.arange(FINE, dtype=jnp.float32).reshape(1, FINE, 1) / FINE
    outer = jnp.arange(COARSE, dtype=jnp.float32).reshape(COARSE, 1, 1) / COARSE
    base = jnp.clip(jax.random.normal(keys[0], (COARSE, FINE, F), jnp.float32), -6.0, 6.0)
    rising = (1.0 + 5.0 * inner) * (0.7 + 0.6 * outer)
    return (base * row_scale * col_scale * rising).astype(jnp.float32)


def draw_tile_counts(key, part):
    keys = jax.random.split(jax.random.fold_in(key, 7), 3)
    limits = jax.random.randint(keys[0], (COARSE, GROUPS_R, 1), max(SLOTS // 3, 1), SLOTS + 1)
    counts = jax.random.randint(keys[1], (COARSE, GROUPS_R, COARSE), 1, limits + 1)
    chosen = jax.random.randint(keys[2], (), 0, COARSE * GROUPS_R * COARSE)
    position = jnp.arange(COARSE * GROUPS_R * COARSE, dtype=jnp.int32).reshape(COARSE, GROUPS_R, COARSE)
    return jnp.where(position == chosen, SLOTS, counts).astype(jnp.int32)


def set_ends(values, key, smallest, largest):
    longest = values.shape.index(max(values.shape))
    spots = []
    for shift in (0, 1):
        where = [jax.random.randint(jax.random.fold_in(key, axis), (), 0, length) for axis, length in enumerate(values.shape)]
        where[longest] = (where[longest] + shift) % values.shape[longest]
        spots.append(tuple(where))
    return values.at[spots[0]].set(smallest).at[spots[1]].set(largest)


def levels(key, dims, cuts, low, top_value):
    loudness, own = 1.0, jax.random.fold_in(key, 6)
    for dim, blocks in cuts:
        heights = jnp.exp(jax.random.uniform(jax.random.fold_in(own, dim), (blocks,), jnp.float32, low / len(cuts), top_value / len(cuts)))
        loudness = loudness * jnp.repeat(heights, dims[dim] // blocks).reshape([-1 if axis == dim else 1 for axis in range(len(dims))])
    return loudness


def scatter_about(own_key, shape, spread, limit, cuts=(), kind=jnp.bfloat16):
    drawn = spread * jax.random.normal(own_key, shape, jnp.float32)
    if cuts:
        drawn = drawn * levels(own_key, shape, cuts, -0.22, 0.18)
    return jnp.clip(drawn, -limit, limit).astype(kind)


def setup_inputs(seed: int = 0) -> dict:
    arg_keys = jax.random.split(jax.random.key(seed), 5)
    features = draw_features(jax.random.fold_in(arg_keys[4], 71), 0)
    tiles = scatter_about(arg_keys[1], (COARSE, GROUPS_R, COARSE, SLOTS, TILE, TILE), (9 * TILE * COARSE // (2 * GROUPS_R)) ** -0.5, 0.1875, ((0, 8), (1, 4)))
    tile_ids = set_ends(jax.random.randint(arg_keys[2], (COARSE, GROUPS_R, COARSE, SLOTS), 0, ROW_TILES * COL_TILES), jax.random.fold_in(arg_keys[2], 1), 0, (ROW_TILES * COL_TILES) - 1).astype(jnp.int32)
    tile_counts = draw_tile_counts(jax.random.fold_in(arg_keys[4], 71), 0)
    return {"features": features, "tiles": tiles, "tile_ids": tile_ids, "tile_counts": tile_counts}


def source_term(running, source_block, matrices, slot_ids, live_count):
    tile_size = matrices.shape[-1]
    slot_count = slot_ids.shape[0]
    row_tiles = running.shape[0]
    columns = source_block.shape[-1]
    col_tiles = source_block.shape[0] // tile_size
    pieces = source_block.reshape(col_tiles, tile_size, columns)
    picked = jnp.take(pieces, slot_ids % col_tiles, axis=0)
    products = jnp.einsum('sij,sjf->sif', matrices.astype(jnp.float32), picked.astype(jnp.float32), precision=lax.Precision.HIGHEST)
    in_use = lax.iota(jnp.int32, slot_count) < live_count
    placement = ((slot_ids // col_tiles)[None, :] == lax.iota(jnp.int32, row_tiles)[:, None]) & in_use[None, :]
    return running + jnp.einsum('rs,sif->rif', placement.astype(jnp.float32), products, precision=lax.Precision.HIGHEST)

def device_partial(dev_tiles, dev_ids, dev_counts, sources):
    zeroed = jnp.zeros((ROW_TILES, TILE, F), jnp.float32)

    def sweep(running, source):
        result = source_term(running, sources[source], dev_tiles[source], dev_ids[source], dev_counts[source])
        return (result, None)
    running, _ = lax.scan(sweep, zeroed, jnp.arange(COARSE, dtype=jnp.int32))
    return running

def reference(features, tiles, tile_ids, tile_counts):
    current = features
    squares = []
    for iteration in range(ITERS):
        rounded = current.astype(jnp.bfloat16).reshape(COARSE, GROUPS_R, NODE_DEV, F)

        def per_coarse(coarse):

            def per_group(running, group):
                sources = rounded[:, group]
                partial_value = device_partial(tiles[coarse, group], tile_ids[coarse, group], tile_counts[coarse, group], sources)
                return (running + partial_value, None)
            start_sum = jnp.zeros((ROW_TILES, TILE, F), jnp.float32)
            running, _ = lax.scan(per_group, start_sum, jnp.arange(GROUPS_R, dtype=jnp.int32))
            return running.reshape(FINE, F)
        product = lax.map(per_coarse, jnp.arange(COARSE, dtype=jnp.int32))
        updated = 0.9 * product + 0.1 * features
        squares.append(jnp.sum((updated - current) ** 2))
        current = updated
    residual_norms = jnp.sqrt(jnp.stack(squares) / (COARSE * FINE * F))
    return (current, residual_norms)
```

```python
import functools

import jax
import jax.numpy as jnp
from jax import lax
from jax.experimental import pallas as pl
from jax.experimental.pallas import tpu as pltpu
from jax.sharding import PartitionSpec as P

ITERS = 3
ALPHA = 0.1
MESH = pl.DeviceIdType.MESH


def kernel(
    nrow, ncol, chunks, depth, ids_hbm, counts_hbm, feat_hbm, tiles_hbm, out_hbm, norm_ref,
    ids, counts, feat, teleport, table, lookup, dense, gathered, acc, current, stage, landed, squares, sums,
    small_sem, feat_sem, tile_sem, table_sem, out_sem, ag_send, ag_recv, d2d_send, rs_send, rs_recv, sq_send, sq_recv,
    *bufs,
):
    nz = ncol // 2
    nodes, feats = feat.shape
    slots = tiles_hbm.shape[1]
    tile = tiles_hbm.shape[-1]
    width = feats // chunks
    row_tiles = nrow * nodes // tile
    col_tiles = nodes // tile
    places = row_tiles * col_tiles
    steps = ITERS * chunks
    r = lax.axis_index("row")
    c = lax.axis_index("col")
    z = c // 2
    core = c % 2
    sibling = z * 2 + 1 - core
    middle = (z == 1) | (z == 2)

    def peer(k):
        if nz == 4:
            return (z, z + 1 - 2 * (z % 2), (z + 2) % 4, 3 - z)[k]
        return (z + k) % nz

    def tile_copy(k, slot):
        return pltpu.make_async_copy(
            tiles_hbm.at[pl.ds(2 * peer(k), 2)], bufs[slot].at[:, pl.ds(0, slots)], tile_sem.at[slot]
        )

    feat_copy = pltpu.make_async_copy(feat_hbm, feat, feat_sem)
    feat_copy.start()
    small_copies = (
        pltpu.make_async_copy(ids_hbm, ids, small_sem.at[0]),
        pltpu.make_async_copy(counts_hbm, counts, small_sem.at[1]),
    )
    for copy in small_copies:
        copy.start()
    for k in range(depth):
        tile_copy(k, k).start()

    barrier = pltpu.get_barrier_semaphore()
    for k in range(1, ncol):
        pl.semaphore_signal(barrier, inc=1, device_id={"col": (c + k) % ncol}, device_id_type=MESH)
    for k in range(1, nrow):
        pl.semaphore_signal(barrier, inc=1, device_id={"row": (r + k) % nrow}, device_id_type=MESH)

    def turn(j):
        lanes = slice(j * tile, (j + 1) * tile)
        teleport[lanes] = feat[:, lanes].T
        for ch in range(j * tile // width, (j + 1) * tile // width):
            gathered[0, ch, c] = teleport[ch * width : (ch + 1) * width].astype(jnp.bfloat16)

    feat_copy.wait()
    turn(0)
    pl.semaphore_wait(barrier, ncol - 1 + nrow - 1)

    def block_copy(n, source, target, send_sem):
        par, ch = n // chunks % 2, n % chunks
        ref = gathered.at[par, ch, source]
        return pltpu.make_async_remote_copy(
            src_ref=ref, dst_ref=ref, send_sem=send_sem, recv_sem=ag_recv.at[par, ch, source],
            device_id={"col": target}, device_id_type=MESH,
        )

    def direct(k, act):
        if nz == 4 and k == 3:
            pl.when(middle)(act)
        else:
            act()

    send_order = [2, 1, 3] if nz == 4 else list(range(1, nz))

    def gather_drain(ch):
        for k in send_order:
            def go(k=k):
                block_copy(ch, c, peer(k) * 2 + core, ag_send.at[ch, k]).wait_send()
            direct(k, go)
        for k in range(nz):
            block_copy(ch, c, sibling, d2d_send.at[ch, k]).wait_send()
        if nz == 4:
            @pl.when(middle)
            def _():
                block_copy(ch, c, sibling, ag_send.at[ch, 0]).wait_send()

    def send(n):
        ch = n % chunks
        if n >= chunks:
            gather_drain(ch)
        for k in send_order:
            def go(k=k):
                block_copy(n, c, peer(k) * 2 + core, ag_send.at[ch, k]).start()
            direct(k, go)
        block_copy(n, c, sibling, d2d_send.at[ch, 0]).start()

    def relay(n, k):
        ch = n % chunks
        source = peer(k) * 2 + core
        block_copy(n, source, sibling, d2d_send.at[ch, k]).wait_recv()
        if nz == 4 and k == 2:
            @pl.when(middle)
            def _():
                block_copy(n, source, 6 * (z - 1) + core, ag_send.at[ch, 0]).start()
        block_copy(n, source, sibling, d2d_send.at[ch, k]).start()

    def part(n, k):
        par, ch = n // chunks % 2, n % chunks
        q = peer(k)
        block_copy(n, q * 2 + 1 - core, sibling, d2d_send.at[ch, 0]).wait_recv()
        source = jnp.concatenate([gathered[par, ch, 2 * q], gathered[par, ch, 2 * q + 1]], axis=1)
        return jnp.dot(source, dense[k], preferred_element_type=jnp.float32)

    def product(n, k):
        ch = n % chunks
        got = part(n, k)
        for j in range(nrow):
            own = got[:, j * nodes : (j + 1) * nodes]
            acc[ch, j] = own if k == 0 else acc[ch, j] + own

    def share_copy(n, k):
        par, ch = n // chunks % 2, n % chunks
        j = r ^ k if nrow == 4 else (r + k) % nrow
        return pltpu.make_async_remote_copy(
            src_ref=stage.at[ch, j], dst_ref=landed.at[par, ch, r],
            send_sem=rs_send.at[ch, k], recv_sem=rs_recv.at[par, ch, r],
            device_id={"row": j}, device_id_type=MESH,
        )

    def finish(n):
        ch = n % chunks
        got = part(n, nz - 1)
        if n >= chunks:
            for k in range(1, nrow):
                share_copy(n, k).wait_send()
        for j in range(nrow):
            total = acc[ch, j] + got[:, j * nodes : (j + 1) * nodes]
            acc[ch, j] = total
            stage[ch, j] = total.astype(jnp.bfloat16)
        for k in range(nrow - 1, 0, -1):
            share_copy(n, k).start()

    def update(n):
        t, ch = n // chunks, n % chunks
        par = t % 2
        rows = slice(ch * width, (ch + 1) * width)
        summed = acc[ch, r]
        for k in range(1, nrow):
            j = r ^ k if nrow == 4 else (r + k) % nrow
            spot = landed.at[par, ch, j]
            pltpu.make_async_remote_copy(
                src_ref=spot, dst_ref=spot, send_sem=rs_send.at[ch, 0],
                recv_sem=rs_recv.at[par, ch, j], device_id={"row": j}, device_id_type=MESH,
            ).wait_recv()
            summed = summed + landed[par, ch, j].astype(jnp.float32)
        here = teleport[rows]
        updated = (1.0 - ALPHA) * summed + ALPHA * here
        before = here if t == 0 else current[rows]
        if t < ITERS - 1:
            gathered[(t + 1) % 2, ch, c] = updated.astype(jnp.bfloat16)
            send(n + chunks)
        current[rows] = updated
        change = (updated - before) ** 2
        change = jnp.sum(change.reshape(width // 8, 8, nodes), axis=0)
        total = change[:, :128]
        for j in range(1, nodes // 128):
            total = total + change[:, j * 128 : (j + 1) * 128]
        squares[t] = total if ch == 0 else squares[t] + total

    def emit(j):
        lanes = slice(j * tile, (j + 1) * tile)
        feat[:, lanes] = current[lanes].T
        copy = pltpu.make_async_copy(feat.at[:, lanes], out_hbm.at[:, lanes], out_sem.at[j])
        copy.start()
        return copy

    zero = jnp.zeros((tile, tile), jnp.bfloat16)
    lane = lax.broadcasted_iota(jnp.int32, (1, table.shape[1]), 1)
    earlier = jnp.where(lane < places, slots, lane - places)

    def find(s, carry):
        own = [ids[s, k] for k in range(slots)]
        live = counts[s]
        wanted = lane
        for k in range(slots):
            wanted = jnp.where(lane == places + k, own[k], wanted)
        limit = jnp.minimum(earlier, live)
        found = jnp.full_like(lane, slots)
        for k in range(slots):
            found = jnp.where((wanted == own[k]) & (limit > k), k, found)
        table[pl.ds(s, 1), :] = found
        return carry

    def build(k, slot):
        q = peer(k)
        buf = bufs[slot]
        tile_copy(k, slot).wait()
        for half in range(2):
            s = 2 * q + half
            for i in range(slots):
                buf[half, i] = buf[half, i].T
            for i in range(1, slots):
                buf[half, i] = buf[half, i] + buf[half, lookup[s, places + i]]
            for i in range(row_tiles):
                for j in range(col_tiles):
                    at = half * nodes + j * tile
                    dense[k, at : at + tile, i * tile : (i + 1) * tile] = buf[half, lookup[s, i * col_tiles + j]]

    send(0)
    if chunks > 1:
        send(1)
    for j in range(1, feats // tile):
        turn(j)
    for slot in range(depth):
        for half in range(2):
            bufs[slot][half, slots] = zero
    for copy in small_copies:
        copy.wait()
    lax.fori_loop(0, ncol, find, 0)
    to_scalars = pltpu.make_async_copy(table, lookup, table_sem)
    to_scalars.start()
    to_scalars.wait()
    if nz == depth:
        builds = [functools.partial(build, k, k) for k in range(nz)]
    else:
        def several(step, carry):
            for slot in range(depth):
                k = step * depth + slot
                build(k, slot)

                @pl.when(k + depth < nz)
                def _():
                    tile_copy(k + depth, slot).start()
            return carry

        lax.fori_loop(0, nz // depth, several, 0)
        builds = []

    def build_some(count):
        for _ in range(min(count, len(builds))):
            builds.pop(0)()

    build_some(2)
    copies = []

    def settle(n):
        update(n)
        done = (n % chunks + 1) * width
        if n // chunks == ITERS - 1 and done % tile == 0:
            copies.append(emit(done // tile - 1))

    if chunks >= 4:
        for m in range(1, steps + 4):
            if m >= 4:
                settle(m - 4)
            elif 1 < m < chunks:
                send(m)
            last, now = m - 2, m - 1
            if 0 <= last < steps:
                relay(last, nz - 1)
            if now < steps:
                for k in range(1, nz - 1):
                    relay(now, k)
                    build_some(1)
            build_some(4)
            if 0 <= last < steps:
                finish(last)
            if now < steps:
                for k in range(nz - 1):
                    product(now, k)
    else:
        build_some(4)
        for n in range(steps):
            for k in range(1, nz):
                if k == nz - 1 and n > 0:
                    settle(n - 1)
                relay(n, k)
                product(n, k - 1)
            finish(n)
        settle(steps - 1)

    size = nrow * ncol
    mine = r * ncol + c
    pad = jnp.zeros((8 - ITERS, 128), jnp.float32)
    sums[mine] = jnp.concatenate([jnp.sum(squares[t], axis=0, keepdims=True) for t in range(ITERS)] + [pad], axis=0)

    def sq_copy(dr, dc, slot):
        return pltpu.make_async_remote_copy(
            src_ref=sums.at[mine], dst_ref=sums.at[slot], send_sem=sq_send.at[dr, dc], recv_sem=sq_recv.at[slot],
            device_id={"row": (r + dr) % nrow, "col": (c + dc) % ncol}, device_id_type=MESH,
        )

    others = [(dr, dc) for dr in range(nrow) for dc in range(ncol) if dr or dc]
    for dr, dc in others:
        sq_copy(dr, dc, mine).start()
    for ch in range(chunks):
        gather_drain(ch)
        for k in range(1, nrow):
            share_copy(ch, k).wait_send()
    for copy in copies:
        copy.wait()
    for dr, dc in others:
        sq_copy(dr, dc, (r + dr) % nrow * ncol + (c + dc) % ncol).wait_recv()
    total = sums[0]
    for j in range(1, size):
        total = total + sums[j]
    count = size * nodes * feats
    norms = jnp.sqrt(jnp.sum(total, axis=1, keepdims=True) / count)
    norm_ref[...] = jnp.broadcast_to(norms, norm_ref.shape)
    for dr, dc in others:
        sq_copy(dr, dc, mine).wait_send()


def local(nrow, ncol, features, tiles, tile_ids, tile_counts):
    own = features[0]
    my_tiles = tiles[0, 0]
    my_ids = tile_ids[0, 0]
    my_counts = tile_counts[0, 0]
    nodes, feats = own.shape
    sources, slots, tile, _ = my_tiles.shape
    nz = ncol // 2
    chunks = 4 if nz == 4 else 2
    depth = 4 if nz == 4 else 2
    width = feats // chunks
    places = (nrow * nodes // tile) * (nodes // tile)
    lanes = pl.cdiv(places + slots, 128) * 128
    bf16, f32 = jnp.bfloat16, jnp.float32
    vmem, smem = pltpu.VMEM, pltpu.SMEM
    dma = pltpu.SemaphoreType.DMA
    anywhere = pl.BlockSpec(memory_space=pl.ANY)
    out, norms = pl.pallas_call(
        functools.partial(kernel, nrow, ncol, chunks, depth),
        out_shape=(jax.ShapeDtypeStruct((nodes, feats), f32), jax.ShapeDtypeStruct((8, 128), f32)),
        in_specs=[anywhere] * 4,
        out_specs=(anywhere, pl.BlockSpec(memory_space=vmem)),
        scratch_shapes=[
            smem((ncol, slots), jnp.int32),
            smem((ncol,), jnp.int32),
            vmem((nodes, feats), f32),
            vmem((feats, nodes), f32),
            vmem((ncol, lanes), jnp.int32),
            smem((ncol, lanes), jnp.int32),
            vmem((nz, 2 * nodes, nrow * nodes), bf16),
            vmem((2, chunks, ncol, width, nodes), bf16),
            vmem((chunks, nrow, width, nodes), f32),
            vmem((feats, nodes), f32),
            vmem((chunks, nrow, width, nodes), bf16),
            vmem((2, chunks, nrow, width, nodes), bf16),
            vmem((ITERS, 8, 128), f32),
            vmem((nrow * ncol, 8, 128), f32),
            dma((2,)),
            dma,
            dma((depth,)),
            dma,
            dma((feats // tile,)),
            dma((chunks, nz)),
            dma((2, chunks, ncol)),
            dma((chunks, nz)),
            dma((chunks, nrow)),
            dma((2, chunks, nrow)),
            dma((nrow, ncol)),
            dma((nrow * ncol,)),
        ]
        + [vmem((2, slots + 1, tile, tile), bf16)] * depth,
        compiler_params=pltpu.CompilerParams(collective_id=0, has_side_effects=True),
    )(my_ids, my_counts, own, my_tiles)
    return (out[None], norms[:ITERS, 0])


def solution(mesh):
    in_specs = (
        P("col", "row", None),
        P("col", "row", None, None, None, None),
        P("col", "row", None, None),
        P("col", "row", None),
    )
    out_specs = (P("col", "row", None), P())
    body = functools.partial(local, mesh.shape["row"], mesh.shape["col"])
    return jax.shard_map(body, mesh=mesh, in_specs=in_specs, out_specs=out_specs, check_vma=False)
```

```python
import functools

import jax
import jax.numpy as jnp
from jax import lax
from jax.experimental import pallas as pl
from jax.experimental.pallas import tpu as pltpu
from jax.sharding import PartitionSpec as P

ITERS = 3
ALPHA = 0.1
MESH = pl.DeviceIdType.MESH


def kernel(
    nrow, ncol, chunks, depth, ids_hbm, counts_hbm, feat_hbm, tiles_hbm, current, norm_ref,
    ids, counts, feat, teleport, table, lookup, dense, gathered, acc, stage, landed, squares, sums,
    small_sem, feat_sem, tile_sem, table_sem, ag_send, ag_recv, d2d_recv, rs_send, rs_recv, sq_send, sq_recv,
    *bufs,
):
    nz = ncol // 2
    nodes, feats = feat.shape
    slots = tiles_hbm.shape[1]
    tile = tiles_hbm.shape[-1]
    width = feats // chunks
    row_tiles = nrow * nodes // tile
    col_tiles = nodes // tile
    places = row_tiles * col_tiles
    steps = ITERS * chunks
    r = lax.axis_index("row")
    c = lax.axis_index("col")
    z = c // 2
    core = c % 2
    sibling = z * 2 + 1 - core
    middle = (z == 1) | (z == 2)

    def peer(k):
        if nz == 4:
            return (z, z + 1 - 2 * (z % 2), (z + 2) % 4, 3 - z)[k]
        return (z + k) % nz

    def tile_copy(k, slot):
        return pltpu.make_async_copy(
            tiles_hbm.at[pl.ds(2 * peer(k), 2)], bufs[slot].at[:, pl.ds(0, slots)], tile_sem.at[slot]
        )

    feat_copy = pltpu.make_async_copy(feat_hbm, feat, feat_sem)
    feat_copy.start()
    small_copies = (
        pltpu.make_async_copy(ids_hbm, ids, small_sem.at[0]),
        pltpu.make_async_copy(counts_hbm, counts, small_sem.at[1]),
    )
    for copy in small_copies:
        copy.start()
    for k in range(depth):
        tile_copy(k, k).start()

    barrier = pltpu.get_barrier_semaphore()
    for k in range(1, ncol):
        pl.semaphore_signal(barrier, inc=1, device_id={"col": (c + k) % ncol}, device_id_type=MESH)
    for k in range(1, nrow):
        pl.semaphore_signal(barrier, inc=1, device_id={"row": (r + k) % nrow}, device_id_type=MESH)

    def turn(j):
        lanes = slice(j * tile, (j + 1) * tile)
        teleport[lanes] = feat[:, lanes].T
        for ch in range(j * tile // width, (j + 1) * tile // width):
            gathered[0, ch, c] = teleport[ch * width : (ch + 1) * width].astype(jnp.bfloat16)

    feat_copy.wait()
    turn(0)
    pl.semaphore_wait(barrier, ncol - 1 + nrow - 1)

    def block_copy(n, source, target, recv_sem, count=None):
        par, ch = n // chunks % 2, n % chunks
        ref = gathered.at[par, ch, source] if count is None else gathered.at[par, ch, pl.ds(0, count)]
        return pltpu.make_async_remote_copy(
            src_ref=ref, dst_ref=ref, send_sem=ag_send.at[ch], recv_sem=recv_sem,
            device_id={"col": target}, device_id_type=MESH,
        )

    def over(n, k):
        return ag_recv.at[n // chunks % 2, n % chunks, k - 1]

    def across(n, k):
        return d2d_recv.at[n // chunks % 2, n % chunks, k // (nz - 1)]

    def direct(k, act):
        if nz == 4 and k == 3:
            pl.when(middle)(act)
        else:
            act()

    send_order = [2, 1, 3] if nz == 4 else list(range(1, nz))

    def gather_drain(ch):
        if nz == 4:
            @pl.when(middle)
            def _():
                block_copy(ch, c, sibling, over(ch, 1), ncol).wait_send()

            @pl.when(jnp.logical_not(middle))
            def _():
                block_copy(ch, c, sibling, over(ch, 1), ncol - 2).wait_send()
        else:
            block_copy(ch, c, sibling, over(ch, 1), ncol - 1).wait_send()

    def send(n):
        if n >= chunks:
            gather_drain(n % chunks)
        for k in send_order:
            def go(k=k):
                block_copy(n, c, peer(k) * 2 + core, over(n, k if nz == 4 else nz - k)).start()
            direct(k, go)
        block_copy(n, c, sibling, across(n, 0)).start()

    def relay(n, k):
        source = peer(k) * 2 + core
        block_copy(n, source, sibling, over(n, k)).wait_recv()
        if nz == 4 and k == 2:
            @pl.when(middle)
            def _():
                block_copy(n, source, 6 * (z - 1) + core, over(n, 3)).start()
        block_copy(n, source, sibling, across(n, k)).start()

    def joined(n, last):
        if last:
            block_copy(n, c, sibling, across(n, nz - 1)).wait_recv()
        else:
            block_copy(n, c, sibling, across(n, 0), nz - 1).wait_recv()

    def part(n, k):
        par, ch = n // chunks % 2, n % chunks
        q = peer(k)
        source = jnp.concatenate([gathered[par, ch, 2 * q], gathered[par, ch, 2 * q + 1]], axis=1)
        return jnp.dot(source, dense[k], preferred_element_type=jnp.float32)

    def product(n, k):
        ch = n % chunks
        got = part(n, k)
        for j in range(nrow):
            own = got[:, j * nodes : (j + 1) * nodes]
            acc[ch, j] = own if k == 0 else acc[ch, j] + own

    def share_copy(n, k):
        par, ch = n // chunks % 2, n % chunks
        j = r ^ k if nrow == 4 else (r + k) % nrow
        return pltpu.make_async_remote_copy(
            src_ref=stage.at[ch, j], dst_ref=landed.at[par, ch, r],
            send_sem=rs_send.at[ch], recv_sem=rs_recv.at[par, ch],
            device_id={"row": j}, device_id_type=MESH,
        )

    def shares(n):
        par, ch = n // chunks % 2, n % chunks
        return pltpu.make_async_remote_copy(
            src_ref=stage.at[ch, pl.ds(0, nrow - 1)], dst_ref=landed.at[par, ch, pl.ds(0, nrow - 1)],
            send_sem=rs_send.at[ch], recv_sem=rs_recv.at[par, ch],
            device_id={"row": (r + 1) % nrow}, device_id_type=MESH,
        )

    def finish(n):
        ch = n % chunks
        joined(n, True)
        got = part(n, nz - 1)
        if n >= chunks:
            shares(n).wait_send()
        for j in range(nrow):
            total = acc[ch, j] + got[:, j * nodes : (j + 1) * nodes]
            acc[ch, j] = total
            stage[ch, j] = total.astype(jnp.bfloat16)
        for k in range(nrow - 1, 0, -1):
            share_copy(n, k).start()

    def update(n):
        t, ch = n // chunks, n % chunks
        par = t % 2
        rows = slice(ch * width, (ch + 1) * width)
        summed = acc[ch, r]
        shares(n).wait_recv()
        for k in range(1, nrow):
            j = r ^ k if nrow == 4 else (r + k) % nrow
            summed = summed + landed[par, ch, j].astype(jnp.float32)
        here = teleport[rows]
        updated = (1.0 - ALPHA) * summed + ALPHA * here
        before = here if t == 0 else current[rows]
        if t < ITERS - 1:
            gathered[(t + 1) % 2, ch, c] = updated.astype(jnp.bfloat16)
            send(n + chunks)
        current[rows] = updated
        change = (updated - before) ** 2
        change = jnp.sum(change.reshape(width // 8, 8, nodes), axis=0)
        total = change[:, :128]
        for j in range(1, nodes // 128):
            total = total + change[:, j * 128 : (j + 1) * 128]
        squares[t] = total if ch == 0 else squares[t] + total

    zero = jnp.zeros((tile, tile), jnp.bfloat16)
    lane = lax.broadcasted_iota(jnp.int32, (1, table.shape[1]), 1)
    earlier = jnp.where(lane < places, slots, lane - places)

    def find(s, carry):
        own = [ids[s, k] for k in range(slots)]
        live = counts[s]
        wanted = lane
        for k in range(slots):
            wanted = jnp.where(lane == places + k, own[k], wanted)
        limit = jnp.minimum(earlier, live)
        found = jnp.full_like(lane, slots)
        for k in range(slots):
            found = jnp.where((wanted == own[k]) & (limit > k), k, found)
        table[pl.ds(s, 1), :] = found
        return carry

    def flip(k, slot):
        buf = bufs[slot]
        tile_copy(k, slot).wait()
        for half in range(2):
            for i in range(slots):
                buf[half, i] = buf[half, i].T

    def build(k, slot):
        q = peer(k)
        buf = bufs[slot]
        for half in range(2):
            s = 2 * q + half
            for i in range(1, slots):
                buf[half, i] = buf[half, i] + buf[half, lookup[s, places + i]]
            for i in range(row_tiles):
                for j in range(col_tiles):
                    at = half * nodes + j * tile
                    dense[k, at : at + tile, i * tile : (i + 1) * tile] = buf[half, lookup[s, i * col_tiles + j]]

    send(0)
    if chunks > 1:
        send(1)
    for copy in small_copies:
        copy.wait()
    lax.fori_loop(0, ncol, find, 0)
    to_scalars = pltpu.make_async_copy(table, lookup, table_sem)
    to_scalars.start()
    for j in range(1, feats // tile):
        turn(j)
    for slot in range(depth):
        for half in range(2):
            bufs[slot][half, slots] = zero
    if nz == depth:
        for k in range(nz):
            flip(k, k)
        to_scalars.wait()
        for k in range(nz):
            build(k, k)
    else:
        def several(step, carry):
            for slot in range(depth):
                k = step * depth + slot
                flip(k, slot)
                build(k, slot)

                @pl.when(k + depth < nz)
                def _():
                    tile_copy(k + depth, slot).start()
            return carry

        to_scalars.wait()
        lax.fori_loop(0, nz // depth, several, 0)

    def settle(n):
        update(n)

    relay_order = [2, 1] if nz == 4 else list(range(1, nz - 1))
    if chunks >= 4:
        for m in range(1, steps + 3):
            last, now = m - 2, m - 1
            if 0 <= last < steps:
                relay(last, nz - 1)
            if now < steps:
                for k in relay_order:
                    relay(now, k)
            if 1 < m + 1 < chunks:
                send(m + 1)
            if 0 <= last < steps:
                finish(last)
            if now < steps:
                joined(now, False)
            for k in range(nz - 1):
                if k == nz - 3 and m >= 3:
                    settle(m - 3)
                if now < steps:
                    product(now, k)
    else:
        for n in range(steps):
            for k in range(1, nz):
                if k == nz - 1 and n > 0:
                    settle(n - 1)
                relay(n, k)
            joined(n, False)
            for k in range(nz - 1):
                product(n, k)
            finish(n)
        settle(steps - 1)

    size = nrow * ncol
    mine = r * ncol + c
    pad = jnp.zeros((8 - ITERS, 128), jnp.float32)
    sums[mine] = jnp.concatenate([jnp.sum(squares[t], axis=0, keepdims=True) for t in range(ITERS)] + [pad], axis=0)

    def sq_copy(j, q, slot, count=None):
        spot = sums.at[slot] if count is None else sums.at[pl.ds(0, count)]
        return pltpu.make_async_remote_copy(
            src_ref=spot, dst_ref=spot, send_sem=sq_send, recv_sem=sq_recv,
            device_id={"row": j, "col": q}, device_id_type=MESH,
        )

    for k in range(nz - 1, -1, -1):
        for side in range(1, -1, -1):
            for dr in range(nrow - 1, -1, -1):
                if k or side or dr:
                    j = r ^ dr if nrow == 4 else (r + dr) % nrow
                    sq_copy(j, peer(k) * 2 + (1 - core if side else core), mine).start()
    for ch in range(chunks):
        gather_drain(ch)
        shares(ch).wait_send()
    sq_copy(r, sibling, mine, size - 1).wait_recv()
    total = sums[0]
    for j in range(1, size):
        total = total + sums[j]
    count = size * nodes * feats
    norms = jnp.sqrt(jnp.sum(total, axis=1, keepdims=True) / count)
    norm_ref[...] = jnp.broadcast_to(norms, norm_ref.shape)
    sq_copy(r, sibling, mine, size - 1).wait_send()


def close(held_ref, norms_ref, out_ref, norm_ref):
    out_ref[0] = held_ref[...].T
    for t in range(ITERS):
        norm_ref[t] = norms_ref[t, 0]


def local(nrow, ncol, features, tiles, tile_ids, tile_counts):
    own = features[0]
    my_tiles = tiles[0, 0]
    my_ids = tile_ids[0, 0]
    my_counts = tile_counts[0, 0]
    nodes, feats = own.shape
    sources, slots, tile, _ = my_tiles.shape
    nz = ncol // 2
    chunks = 4 if nz == 4 else 2
    depth = 4 if nz == 4 else 2
    width = feats // chunks
    places = (nrow * nodes // tile) * (nodes // tile)
    lanes = pl.cdiv(places + slots, 128) * 128
    bf16, f32 = jnp.bfloat16, jnp.float32
    vmem, smem = pltpu.VMEM, pltpu.SMEM
    dma = pltpu.SemaphoreType.DMA
    anywhere = pl.BlockSpec(memory_space=pltpu.HBM)
    out, norms = pl.pallas_call(
        functools.partial(kernel, nrow, ncol, chunks, depth),
        out_shape=(jax.ShapeDtypeStruct((feats, nodes), f32), jax.ShapeDtypeStruct((8, 128), f32)),
        in_specs=[anywhere] * 4,
        out_specs=(pl.BlockSpec(memory_space=vmem), pl.BlockSpec(memory_space=vmem)),
        scratch_shapes=[
            smem((ncol, slots), jnp.int32),
            smem((ncol,), jnp.int32),
            vmem((nodes, feats), f32),
            vmem((feats, nodes), f32),
            vmem((ncol, lanes), jnp.int32),
            smem((ncol, lanes), jnp.int32),
            vmem((nz, 2 * nodes, nrow * nodes), bf16),
            vmem((2, chunks, ncol, width, nodes), bf16),
            vmem((chunks, nrow, width, nodes), f32),
            vmem((chunks, nrow, width, nodes), bf16),
            vmem((2, chunks, nrow, width, nodes), bf16),
            vmem((ITERS, 8, 128), f32),
            vmem((nrow * ncol, 8, 128), f32),
            dma((2,)),
            dma,
            dma((depth,)),
            dma,
            dma((chunks,)),
            dma((2, chunks, nz - 1)),
            dma((2, chunks, 2)),
            dma((chunks,)),
            dma((2, chunks)),
            dma,
            dma,
        ]
        + [vmem((2, slots + 1, tile, tile), bf16)] * depth,
        compiler_params=pltpu.CompilerParams(
            collective_id=0, has_side_effects=True, vmem_limit_bytes=(24 if nz == 4 else 60) * 2**20
        ),
    )(*(pltpu.with_memory_space_constraint(x, pltpu.HBM) for x in (my_ids, my_counts, own, my_tiles)))
    return tuple(
        pl.pallas_call(
            close,
            out_shape=(jax.ShapeDtypeStruct((1, nodes, feats), f32), jax.ShapeDtypeStruct((ITERS,), f32)),
            in_specs=[pl.BlockSpec(memory_space=vmem), pl.BlockSpec(memory_space=vmem)],
            out_specs=(pl.BlockSpec(memory_space=vmem), pl.BlockSpec(memory_space=smem)),
            compiler_params=pltpu.CompilerParams(vmem_limit_bytes=4 * 2**20),
        )(out, norms)
    )


def solution(mesh):
    in_specs = (
        P("col", "row", None),
        P("col", "row", None, None, None, None),
        P("col", "row", None, None),
        P("col", "row", None),
    )
    out_specs = (P("col", "row", None), P())
    body = functools.partial(local, mesh.shape["row"], mesh.shape["col"])
    return jax.shard_map(body, mesh=mesh, in_specs=in_specs, out_specs=out_specs, check_vma=False)
```
